32 devices in a mesh: trial: 4 (over y, x), fsdp: 2 (over core), cols: 4 (over z).
Axes of the slice: x: 2, y: 2, z: 4, core: 2. Of those that a mesh axis runs over, the one named last changes fastest.
Arguments:
- train_gate: bfloat16 [8192, 8192], P(('trial', 'fsdp'), 'cols'), parts along dimension 0, may hold values from -0.1875 to 0.1875
- low_gate: bfloat16 [8192, 16], P(('trial', 'fsdp')), parts along dimension 0, may hold values from -0.125 to 0.125
- high_gate: bfloat16 [64, 8192], P('trial', 'cols'), parts along dimension 0, may hold values from -1.5 to 1.5
- train_up: bfloat16 [8192, 8192], P(('trial', 'fsdp'), 'cols'), parts along dimension 0, may hold values from -0.1875 to 0.1875
- low_up: bfloat16 [8192, 16], P(('trial', 'fsdp')), parts along dimension 0, may hold values from -0.125 to 0.125
- high_up: bfloat16 [64, 8192], P('trial', 'cols'), parts along dimension 0, may hold values from -1.5 to 1.5
- norm_gain: float32 [8192], P(('trial', 'fsdp')), parts along dimension 0, may hold values from 0.25 to 1.75
Outputs:
- ready_gate: bfloat16 [8192, 8192], P('trial', 'cols'), parts along dimension 0
- ready_up: bfloat16 [8192, 8192], P('trial', 'cols'), parts along dimension 0
- column_gate: float32 [32768], P(('trial', 'cols')), parts along dimension 0
- column_up: float32 [32768], P(('trial', 'cols')), parts along dimension 0
The draws below stay inside these ranges and needn't reach their ends.
There are 4 independent parts, one for each index of `trial`. The reference program is written for one: setup_inputs(seed, part) draws one part's arguments, and reference() takes and returns one part's arrays. A program takes and returns all parts, laid end to end along the dimension named above; each array names one. Nothing has to cross between parts.
All inputs are finite; a program needn't handle non-finite values. Where the reference program divides by a largest or mean magnitude, that divisor is 1e-20 or more.
Results may differ from the reference program's by a relative error of at most 0.001.
Values may be sent and summed in bfloat16 or wider, within the bound.
A program may use at most 128 MiB of HBM per device.

```python
import jax
import jax.numpy as jnp

D_MODEL = 2048
D_INNER = 8192
RANK = 16


def spiked(drawn, own_key, source, target, shards_of, factor):
    owner, partner = [(jnp.arange(drawn.shape[axis_at]) // (drawn.shape[axis_at] // shards_of)).reshape([-1 if axis == axis_at else 1 for axis in range(drawn.ndim)]) for axis_at in (source, target)]
    chosen = jax.random.permutation(own_key, shards_of)[partner]
    strong = (owner == chosen) | (owner == (partner + shards_of // 2) % shards_of)
    return jnp.where(strong, factor * drawn, drawn)


def levels(key, shape, split, least, high):
    def one(dim, parts):
        draws = jax.random.uniform(jax.random.fold_in(jax.random.fold_in(key, 6), dim), (parts,), jnp.float32, least / len(split), high / len(split))
        return jnp.repeat(jnp.exp(draws), shape[dim] // parts).reshape((-1,) + (1,) * (len(shape) - dim - 1))

    factor_of = one(*split[0])
    for cut in split[1:]:
        factor_of = factor_of * one(*cut)
    return factor_of


def gaussian(own_key, shape, spread, bound, shards=(), held_as=jnp.bfloat16):
    drawn = jax.random.normal(own_key, shape, jnp.float32) * spread
    if len(shards) > 0:
        drawn = levels(own_key, shape, shards, -0.22, 0.18) * drawn
    return jnp.clip(drawn, min=-bound, max=bound).astype(held_as)


def gaussian_with(stream_key, shape, spread, bound, split, heavy, kind=jnp.bfloat16):
    array = spread * jax.random.normal(stream_key, shape, jnp.float32)
    if split:
        array = array * levels(stream_key, shape, split, -0.22, 0.18)
    return jnp.clip(spiked(array, jax.random.fold_in(stream_key, 3), *heavy), -bound, bound).astype(kind)


def setup_inputs(seed: int = 0, part: int = 0) -> dict:
    seeds = jax.random.split(jax.random.key(seed), 8)
    own_keys = jax.random.split(jax.random.fold_in(seeds[7], part), 8)
    train_gate = gaussian_with(own_keys[0], (D_MODEL, D_INNER), D_MODEL ** -0.5, 0.1875, ((0, 2), (1, 4)), (0, 1, 4, 2.0))
    low_gate = gaussian(own_keys[1], (D_MODEL, RANK), D_MODEL ** -0.5, 0.125, ((0, 2),))
    high_gate = gaussian(own_keys[2], (RANK, D_INNER), RANK ** -0.5, 1.5, ((1, 4),))
    train_up = gaussian_with(own_keys[3], (D_MODEL, D_INNER), D_MODEL ** -0.5, 0.1875, ((0, 2), (1, 4)), (0, 1, 4, 2.0))
    low_up = gaussian(own_keys[4], (D_MODEL, RANK), D_MODEL ** -0.5, 0.125, ((0, 2),))
    high_up = gaussian(own_keys[5], (RANK, D_INNER), RANK ** -0.5, 1.5, ((1, 4),))
    norm_gain = jnp.clip(1.0 + 0.15 * jax.random.normal(own_keys[6], (D_MODEL,), jnp.float32), 0.25, 1.75)
    return {"train_gate": train_gate, "low_gate": low_gate, "high_gate": high_gate, "train_up": train_up, "low_up": low_up, "high_up": high_up, "norm_gain": norm_gain}


mix_rate = 1.0


def reference(train_gate, low_gate, high_gate, train_up, low_up, high_up, norm_gain):
    latest_gate = train_gate.astype(jnp.float32) + mix_rate * jnp.dot(low_gate, high_gate, preferred_element_type=jnp.float32)
    latest_up = train_up.astype(jnp.float32) + mix_rate * jnp.dot(low_up, high_up, preferred_element_type=jnp.float32)
    latest_gained_gate = latest_gate * norm_gain[:, None]
    latest_gained_up = latest_up * norm_gain[:, None]
    column_gate = jnp.max(jnp.abs(latest_gained_gate), axis=0)
    ready_gate = (latest_gained_gate / column_gate).astype(jnp.bfloat16)
    column_up = jnp.max(jnp.abs(latest_gained_up), axis=0)
    ready_up = (latest_gained_up / column_up).astype(jnp.bfloat16)
    return ready_gate, ready_up, column_gate, column_up
```

```python
import functools

import jax
import jax.numpy as jnp
from jax import lax
from jax.experimental import pallas as pl
from jax.experimental.pallas import tpu as pltpu
from jax.sharding import PartitionSpec as P


BLOCK = 128
TILE = 256
STAT_ROWS = 8


def in_hbm(x):
    return pltpu.with_memory_space_constraint(x, pltpu.HBM)


def in_vmem(x):
    return pltpu.with_memory_space_constraint(x, pltpu.VMEM)


VMEM_SPEC = pl.BlockSpec(memory_space=pltpu.VMEM)
HBM_SPEC = pl.BlockSpec(memory_space=pl.ANY)


def spread_rows(low_t, gain, low_rows, gain_rows, at):
    rows = low_t.shape[1]
    low_rows[at : at + rows, :] = low_t.astype(jnp.float32).T.astype(jnp.bfloat16)
    if gain is not None:
        gain_rows[at : at + rows, :] = jnp.broadcast_to(gain, (128, rows)).T


def gained_tile(raw, low, high, gain):
    added = jnp.dot(low, high, preferred_element_type=jnp.float32)
    latest = raw.astype(jnp.float32) + added
    return latest * jnp.concatenate([gain] * (raw.shape[1] // 128), axis=1)


def own_kernel(chunks, gate_hbm, up_hbm, *refs):
    small_hbm = refs[:5]
    gained_gate, gained_up, stat, high_gate, high_up = refs[5:10]
    pieces = refs[10 : 10 + len(chunks)]
    gate_buf, low_gate_t, low_up_t, gain, low_rows, gain_rows, top, small_sems, gate_sems, up_sems = refs[
        10 + len(chunks) :
    ]
    rows, columns = gate_hbm.shape
    block = min(BLOCK, rows)
    tile = min(TILE, columns)

    def gate_copy(i):
        at = pl.multiple_of(i * block, block)
        return pltpu.make_async_copy(
            gate_hbm.at[pl.ds(at, block), :], gate_buf.at[pl.ds(at, block), :], gate_sems.at[i]
        )

    def up_copy(piece, start, i):
        at = pl.multiple_of(i * block, block)
        return pltpu.make_async_copy(
            up_hbm.at[pl.ds(start + at, block), :], piece.at[pl.ds(at, block), :], up_sems.at[start // block + i]
        )

    small = [
        pltpu.make_async_copy(source, target, small_sems.at[n])
        for n, (source, target) in enumerate(zip(small_hbm, (low_gate_t, low_up_t, gain, high_gate, high_up)))
    ]
    for copy in small:
        copy.start()
    for i in range(rows // block):
        gate_copy(i).start()
    for piece, (start, size) in zip(pieces, chunks):
        for i in range(size // block):
            up_copy(piece, start, i).start()
    for copy in small:
        copy.wait()
    spread_rows(low_gate_t[...], gain[...], low_rows, gain_rows, 0)
    spread_rows(low_up_t[...], None, low_rows, gain_rows, rows)
    top[...] = jnp.zeros_like(top)

    def merge_block(raw_ref, raw_at, at, low_at, high_ref, gained, top_at):
        low = low_rows[pl.ds(low_at + at, block), :]
        gain_block = gain_rows[pl.ds(at, block), :]
        for c in range(0, columns, tile):
            value = gained_tile(
                raw_ref[pl.ds(raw_at, block), c : c + tile], low, high_ref[:, c : c + tile], gain_block
            )
            gained[pl.ds(at, block), c : c + tile] = value
            best = jnp.max(jnp.abs(value).reshape(block // 8, 8, tile), axis=0)
            top[top_at : top_at + 8, c : c + tile] = jnp.maximum(top[top_at : top_at + 8, c : c + tile], best)

    @pl.loop(0, rows // block)
    def _(i):
        gate_copy(i).wait()
        at = pl.multiple_of(i * block, block)
        merge_block(gate_buf, at, at, 0, high_gate, gained_gate, 0)

    for piece, (start, size) in zip(pieces, chunks):

        @pl.loop(0, size // block)
        def _(i, piece=piece, start=start):
            up_copy(piece, start, i).wait()
            at = pl.multiple_of(i * block, block)
            merge_block(piece, at, start + at, rows, high_up, gained_up, 8)

    stat[...] = jnp.zeros_like(stat)
    stat[0:1, :] = jnp.max(top[0:8, :], axis=0, keepdims=True)
    stat[1:2, :] = jnp.max(top[8:16, :], axis=0, keepdims=True)
    stat[2:3, :rows] = gain[...]


def own(train_gate, train_up, low_gate_t, low_up_t, gain, high_gate, high_up, chunks):
    rows, columns = train_gate.shape
    rank = high_gate.shape[0]
    block = min(BLOCK, rows)
    return pl.pallas_call(
        functools.partial(own_kernel, chunks),
        out_shape=(
            pltpu.VMEM((rows, columns), jnp.float32),
            pltpu.VMEM((rows, columns), jnp.float32),
            pltpu.VMEM((STAT_ROWS, columns), jnp.float32),
            pltpu.VMEM((rank, columns), jnp.bfloat16),
            pltpu.VMEM((rank, columns), jnp.bfloat16),
            *[pltpu.VMEM((size, columns), jnp.bfloat16) for _, size in chunks],
        ),
        in_specs=[HBM_SPEC] * 7,
        out_specs=(VMEM_SPEC,) * (5 + len(chunks)),
        scratch_shapes=[
            pltpu.VMEM((rows, columns), jnp.bfloat16),
            pltpu.VMEM((rank, rows), jnp.bfloat16),
            pltpu.VMEM((rank, rows), jnp.bfloat16),
            pltpu.VMEM((1, rows), jnp.float32),
            pltpu.VMEM((2 * rows, rank), jnp.bfloat16),
            pltpu.VMEM((rows, 128), jnp.float32),
            pltpu.VMEM((16, columns), jnp.float32),
            pltpu.SemaphoreType.DMA((5,)),
            pltpu.SemaphoreType.DMA((rows // block,)),
            pltpu.SemaphoreType.DMA((rows // block,)),
        ],
        compiler_params=pltpu.CompilerParams(vmem_limit_bytes=12 * 1024 * 1024),
        cost_estimate=pl.CostEstimate(
            flops=32 * rows * columns * rank, bytes_accessed=4 * rows * columns, transcendentals=0
        ),
    )(*map(in_hbm, (train_gate, train_up, low_gate_t, low_up_t, gain, high_gate, high_up)))


def write_rows(stage, slot, out_hbm, start, size, sem):
    return pltpu.make_async_copy(stage.at[pl.ds(slot, size), :], out_hbm.at[pl.ds(start, size), :], sem)


def scale_partner(raw, low_rows, low_at, gain_rows, gain_at, high, scale, stage, slot, out_hbm, start, sems, sem_at):
    size, columns = raw.shape
    block = min(BLOCK, size)
    tile = min(TILE, columns)

    @pl.loop(0, size // block)
    def _(i):
        at = pl.multiple_of(i * block, block)
        low = low_rows[pl.ds(low_at + at, block), :]
        gain_block = gain_rows[pl.ds(gain_at + at, block), :]
        for c in range(0, columns, tile):
            value = gained_tile(raw[pl.ds(at, block), c : c + tile], low, high[:, c : c + tile], gain_block)
            scaled = value.reshape(block // 8, 8, tile) * scale[:, c : c + tile][None]
            stage[pl.ds(slot + at, block), c : c + tile] = scaled.reshape(block, tile).astype(jnp.bfloat16)
        write_rows(stage, slot + at, out_hbm, start + at, block, sems.at[sem_at + i]).start()


def scale_own(gained, scale, stage, slot, out_hbm, start, sems, sem_at):
    size, columns = gained.shape
    block = min(BLOCK, size)
    tile = min(TILE, columns)

    @pl.loop(0, size // block)
    def _(i):
        at = pl.multiple_of(i * block, block)
        for c in range(0, columns, tile):
            value = gained[pl.ds(at, block), c : c + tile].reshape(block // 8, 8, tile)
            scaled = (value * scale[:, c : c + tile][None]).reshape(block, tile)
            stage[pl.ds(slot + at, block), c : c + tile] = scaled.astype(jnp.bfloat16)
        write_rows(stage, slot + at, out_hbm, start + at, block, sems.at[sem_at + i]).start()


def wait_rows(stage, slot, out_hbm, start, size, sems, sem_at):
    block = min(BLOCK, size)

    @pl.loop(0, size // block)
    def _(i):
        at = pl.multiple_of(i * block, block)
        write_rows(stage, slot + at, out_hbm, start + at, block, sems.at[sem_at + i]).wait()


def first_kernel(parts, *refs):
    gained_gate, gained_up, high_gate = refs[:3]
    stats = refs[3 : 3 + parts]
    others = parts - 1
    raws = refs[3 + parts : 3 + parts + others]
    low_gates = refs[3 + parts + others : 3 + parts + 2 * others]
    low_ups = refs[3 + parts + 2 * others : 3 + parts + 3 * others]
    rest = refs[3 + parts + 3 * others :]
    ready_gate, ready_up, column_gate, column_up, low_up_rows, gain_rows, scale_up = rest[:7]
    scale_gate, low_gate_rows, stage, sems = rest[7:]
    rows, columns = gained_gate.shape
    block = min(BLOCK, rows)
    blocks = rows // block
    me = lax.axis_index("fsdp")

    best = stats[0][0:2, :]
    for stat in stats[1:]:
        best = jnp.maximum(best, stat[0:2, :])
    column_gate[...] = best[0:1, :]
    column_up[...] = best[1:2, :]
    scale_gate[...] = jnp.broadcast_to(1.0 / best[0:1, :], (8, columns))
    scale_up[...] = jnp.broadcast_to(1.0 / best[1:2, :], (8, columns))

    start = pl.multiple_of(me * rows, rows)
    scale_own(gained_gate, scale_gate, stage, 0, ready_gate, start, sems, 0)
    for k in range(others):
        spread_rows(low_gates[k][...], stats[k + 1][2:3, :rows], low_gate_rows, gain_rows, k * rows)
        spread_rows(low_ups[k][...], None, low_up_rows, gain_rows, k * rows)
        there = pl.multiple_of(lax.rem(me - (k + 1) + parts, parts) * rows, rows)
        scale_partner(
            raws[k], low_gate_rows, k * rows, gain_rows, k * rows, high_gate, scale_gate,
            stage, (k + 1) * rows, ready_gate, there, sems, (k + 1) * blocks,
        )
    scale_own(gained_up, scale_up, stage, parts * rows, ready_up, start, sems, parts * blocks)
    wait_rows(stage, 0, ready_gate, start, rows, sems, 0)
    for k in range(others):
        there = pl.multiple_of(lax.rem(me - (k + 1) + parts, parts) * rows, rows)
        wait_rows(stage, (k + 1) * rows, ready_gate, there, rows, sems, (k + 1) * blocks)
    wait_rows(stage, parts * rows, ready_up, start, rows, sems, parts * blocks)


def first(gained_gate, gained_up, stats, raws, low_gates, low_ups, high_gate):
    parts = len(stats)
    others = parts - 1
    rows, columns = gained_gate.shape
    rank = high_gate.shape[0]
    blocks = rows // min(BLOCK, rows)
    return pl.pallas_call(
        functools.partial(first_kernel, parts),
        out_shape=(
            pltpu.HBM((parts * rows, columns), jnp.bfloat16),
            pltpu.HBM((parts * rows, columns), jnp.bfloat16),
            jax.ShapeDtypeStruct((1, columns), jnp.float32),
            jax.ShapeDtypeStruct((1, columns), jnp.float32),
            pltpu.VMEM((others * rows, rank), jnp.bfloat16),
            pltpu.VMEM((others * rows, 128), jnp.float32),
            pltpu.VMEM((8, columns), jnp.float32),
        ),
        in_specs=[VMEM_SPEC] * (3 + parts + 3 * others),
        out_specs=(HBM_SPEC, HBM_SPEC) + (VMEM_SPEC,) * 5,
        scratch_shapes=[
            pltpu.VMEM((8, columns), jnp.float32),
            pltpu.VMEM((others * rows, rank), jnp.bfloat16),
            pltpu.VMEM(((parts + 1) * rows, columns), jnp.bfloat16),
            pltpu.SemaphoreType.DMA(((parts + 1) * blocks,)),
        ],
        compiler_params=pltpu.CompilerParams(vmem_limit_bytes=18 * 1024 * 1024),
        cost_estimate=pl.CostEstimate(
            flops=16 * parts * rows * columns * rank, bytes_accessed=4 * parts * rows * columns, transcendentals=0
        ),
    )(
        in_vmem(gained_gate), in_vmem(gained_up), in_vmem(high_gate),
        *map(in_vmem, stats), *map(in_vmem, raws), *map(in_vmem, low_gates), *map(in_vmem, low_ups),
    )


def later_kernel(parts, rows, offset, *refs):
    others = parts - 1
    raws = refs[:others]
    low_rows, gain_rows, scale, high, _, ready, stage, sems = refs[others:]
    size = raws[0].shape[0]
    blocks = size // min(BLOCK, size)
    me = lax.axis_index("fsdp")
    for k in range(others):
        there = pl.multiple_of(lax.rem(me - (k + 1) + parts, parts) * rows + offset, min(BLOCK, size))
        scale_partner(
            raws[k], low_rows, k * rows + offset, gain_rows, k * rows + offset, high, scale,
            stage, k * size, ready, there, sems, k * blocks,
        )
    for k in range(others):
        there = pl.multiple_of(lax.rem(me - (k + 1) + parts, parts) * rows + offset, min(BLOCK, size))
        wait_rows(stage, k * size, ready, there, size, sems, k * blocks)


def later(ready, raws, low_rows, gain_rows, scale, high, rows, offset):
    others = len(raws)
    size, columns = raws[0].shape
    rank = high.shape[0]
    blocks = size // min(BLOCK, size)
    return pl.pallas_call(
        functools.partial(later_kernel, others + 1, rows, offset),
        out_shape=pltpu.HBM(ready.shape, ready.dtype),
        in_specs=[VMEM_SPEC] * (others + 4) + [HBM_SPEC],
        out_specs=HBM_SPEC,
        input_output_aliases={others + 4: 0},
        scratch_shapes=[
            pltpu.VMEM((others * size, columns), jnp.bfloat16),
            pltpu.SemaphoreType.DMA((others * blocks,)),
        ],
        compiler_params=pltpu.CompilerParams(vmem_limit_bytes=8 * 1024 * 1024),
        cost_estimate=pl.CostEstimate(
            flops=16 * others * size * columns * rank, bytes_accessed=4 * others * size * columns, transcendentals=0
        ),
    )(*map(in_vmem, raws), in_vmem(low_rows), in_vmem(gain_rows), in_vmem(scale), in_vmem(high), in_hbm(ready))


def chunks_of(rows):
    block = min(BLOCK, rows)
    blocks = rows // block
    first_size = block * max(1, (blocks * 5 + 7) // 8)
    return ((0, first_size), (first_size, rows - first_size)) if first_size < rows else ((0, rows),)


def solution(mesh):
    parts = mesh.shape["fsdp"]

    def around(x):
        return [
            lax.ppermute(x, "fsdp", [(i, (i + k) % parts) for i in range(parts)]) for k in range(1, parts)
        ]

    def per_device(train_gate, low_gate, high_gate, train_up, low_up, high_up, norm_gain):
        rows = train_gate.shape[0]
        chunks = chunks_of(rows)
        gates = around(train_gate)
        low_gates = around(low_gate.T)
        low_ups = around(low_up.T)
        gained_gate, gained_up, stat, high_gate, high_up, *pieces = own(
            train_gate, train_up, low_gate.T, low_up.T, norm_gain.reshape(1, -1), high_gate, high_up, chunks
        )
        stats = [stat] + around(stat)
        ups = [around(piece) for piece in pieces]
        ready_gate, ready_up, column_gate, column_up, low_up_rows, gain_rows, scale_up = first(
            gained_gate, gained_up, stats, gates, low_gates, low_ups, high_gate
        )
        for n, (offset, _) in enumerate(chunks):
            ready_up = later(ready_up, ups[n], low_up_rows, gain_rows, scale_up, high_up, rows, offset)
        return ready_gate, ready_up, column_gate.reshape(-1), column_up.reshape(-1)

    placed = (
        P(("trial", "fsdp"), "cols"),
        P(("trial", "fsdp"), None),
        P("trial", "cols"),
        P(("trial", "fsdp"), "cols"),
        P(("trial", "fsdp"), None),
        P("trial", "cols"),
        P(("trial", "fsdp")),
    )
    return jax.shard_map(
        per_device,
        mesh=mesh,
        in_specs=placed,
        out_specs=(
            P("trial", "cols"),
            P("trial", "cols"),
            P(("trial", "cols")),
            P(("trial", "cols")),
        ),
        check_vma=False,
    )
```

```python
import functools

import jax
import jax.numpy as jnp
from jax import lax
from jax.experimental import pallas as pl
from jax.experimental.pallas import tpu as pltpu
from jax.sharding import PartitionSpec as P


BLOCK = 128
TILE = 256
STAT_ROWS = 8
UNROLL = 4


def in_hbm(x):
    return pltpu.with_memory_space_constraint(x, pltpu.HBM)


def in_vmem(x):
    return pltpu.with_memory_space_constraint(x, pltpu.VMEM)


VMEM_SPEC = pl.BlockSpec(memory_space=pltpu.VMEM)
HBM_SPEC = pl.BlockSpec(memory_space=pl.ANY)


def spread_rows(low_t, gain, low_rows, gain_rows, at):
    rows = low_t.shape[1]
    low_rows[at : at + rows, :] = low_t.astype(jnp.float32).T.astype(jnp.bfloat16)
    if gain is not None:
        gain_rows[at : at + rows, :] = jnp.broadcast_to(gain, (128, rows)).T


def gained_tile(raw, low, high, gain):
    added = jnp.dot(low, high, preferred_element_type=jnp.float32)
    latest = raw.astype(jnp.float32) + added
    return latest * jnp.concatenate([gain] * (raw.shape[1] // 128), axis=1)


def in_groups(blocks, limit, *stages):
    group = max(g for g in range(1, limit + 1) if blocks % g == 0)

    @pl.loop(0, blocks // group)
    def _(n):
        for stage in stages:
            for g in range(group):
                stage(n * group + g)


def own_kernel(chunks, gate_hbm, up_hbm, *refs):
    small_hbm = refs[:5]
    gained_gate, gained_up, stat, high_gate, high_up = refs[5:10]
    pieces = refs[10 : 10 + len(chunks)]
    gate_buf, low_gate_t, low_up_t, gain, low_rows, gain_rows, top, small_sems, gate_sems, up_sems = refs[
        10 + len(chunks) :
    ]
    rows, columns = gate_hbm.shape
    block = min(BLOCK, rows)
    tile = min(TILE, columns)

    def gate_copy(i):
        at = pl.multiple_of(i * block, block)
        return pltpu.make_async_copy(
            gate_hbm.at[pl.ds(at, block), :], gate_buf.at[pl.ds(at, block), :], gate_sems.at[i]
        )

    def up_copy(piece, start, i):
        at = pl.multiple_of(i * block, block)
        return pltpu.make_async_copy(
            up_hbm.at[pl.ds(start + at, block), :], piece.at[pl.ds(at, block), :], up_sems.at[start // block + i]
        )

    small = [
        pltpu.make_async_copy(source, target, small_sems.at[n])
        for n, (source, target) in enumerate(zip(small_hbm, (low_gate_t, low_up_t, gain, high_gate, high_up)))
    ]
    for copy in small:
        copy.start()
    for i in range(rows // block):
        gate_copy(i).start()
    for copy in small:
        copy.wait()
    spread_rows(low_gate_t[...], gain[...], low_rows, gain_rows, 0)
    spread_rows(low_up_t[...], None, low_rows, gain_rows, rows)
    for piece, (start, size) in zip(pieces, chunks):
        for i in range(size // block):
            up_copy(piece, start, i).start()
    top[...] = jnp.zeros_like(top)

    def merge_block(raw_ref, raw_at, start, low_at, high_ref, gained, top_at):
        at = start + raw_at
        low = low_rows[pl.ds(low_at + at, block), :]
        gain_block = gain_rows[pl.ds(at, block), :]
        for c in range(0, columns, tile):
            value = gained_tile(
                raw_ref[pl.ds(raw_at, block), c : c + tile], low, high_ref[:, c : c + tile], gain_block
            )
            gained[pl.ds(at, block), c : c + tile] = value
            best = jnp.max(jnp.abs(value).reshape(block // 8, 8, tile), axis=0)
            top[top_at : top_at + 8, c : c + tile] = jnp.maximum(top[top_at : top_at + 8, c : c + tile], best)

    in_groups(
        rows // block,
        UNROLL,
        lambda i: gate_copy(i).wait(),
        lambda i: merge_block(gate_buf, pl.multiple_of(i * block, block), 0, 0, high_gate, gained_gate, 0),
    )
    for piece, (start, size) in zip(pieces, chunks):
        in_groups(
            size // block,
            UNROLL,
            lambda i: up_copy(piece, start, i).wait(),
            lambda i: merge_block(piece, pl.multiple_of(i * block, block), start, rows, high_up, gained_up, 8),
        )

    stat[...] = jnp.zeros_like(stat)
    stat[0:1, :] = jnp.max(top[0:8, :], axis=0, keepdims=True)
    stat[1:2, :] = jnp.max(top[8:16, :], axis=0, keepdims=True)
    stat[2:3, :rows] = gain[...]


def own(train_gate, train_up, low_gate_t, low_up_t, gain, high_gate, high_up, chunks):
    rows, columns = train_gate.shape
    rank = high_gate.shape[0]
    block = min(BLOCK, rows)
    return pl.pallas_call(
        functools.partial(own_kernel, chunks),
        out_shape=(
            pltpu.VMEM((rows, columns), jnp.float32),
            pltpu.VMEM((rows, columns), jnp.float32),
            pltpu.VMEM((STAT_ROWS, columns), jnp.float32),
            pltpu.VMEM((rank, columns), jnp.bfloat16),
            pltpu.VMEM((rank, columns), jnp.bfloat16),
            *[pltpu.VMEM((size, columns), jnp.bfloat16) for _, size in chunks],
        ),
        in_specs=[HBM_SPEC] * 7,
        out_specs=(VMEM_SPEC,) * (5 + len(chunks)),
        scratch_shapes=[
            pltpu.VMEM((rows, columns), jnp.bfloat16),
            pltpu.VMEM((rank, rows), jnp.bfloat16),
            pltpu.VMEM((rank, rows), jnp.bfloat16),
            pltpu.VMEM((1, rows), jnp.float32),
            pltpu.VMEM((2 * rows, rank), jnp.bfloat16),
            pltpu.VMEM((rows, 128), jnp.float32),
            pltpu.VMEM((16, columns), jnp.float32),
            pltpu.SemaphoreType.DMA((5,)),
            pltpu.SemaphoreType.DMA((rows // block,)),
            pltpu.SemaphoreType.DMA((rows // block,)),
        ],
        compiler_params=pltpu.CompilerParams(vmem_limit_bytes=12 * 1024 * 1024),
        cost_estimate=pl.CostEstimate(
            flops=32 * rows * columns * rank, bytes_accessed=4 * rows * columns, transcendentals=0
        ),
    )(*map(in_hbm, (train_gate, train_up, low_gate_t, low_up_t, gain, high_gate, high_up)))


def write_rows(stage, slot, out_hbm, start, size, sem):
    return pltpu.make_async_copy(stage.at[pl.ds(slot, size), :], out_hbm.at[pl.ds(start, size), :], sem)


def scale_partner(raw, low_rows, low_at, gain_rows, gain_at, high, scale, stage, slot, out_hbm, start, sems, sem_at):
    size, columns = raw.shape
    block = min(BLOCK, size)
    tile = min(TILE, columns)

    def merge(i):
        at = pl.multiple_of(i * block, block)
        low = low_rows[pl.ds(low_at + at, block), :]
        gain_block = gain_rows[pl.ds(gain_at + at, block), :]
        for c in range(0, columns, tile):
            value = gained_tile(raw[pl.ds(at, block), c : c + tile], low, high[:, c : c + tile], gain_block)
            scaled = value.reshape(block // 8, 8, tile) * scale[:, c : c + tile][None]
            stage[pl.ds(slot + at, block), c : c + tile] = scaled.reshape(block, tile).astype(jnp.bfloat16)

    def send(i):
        at = pl.multiple_of(i * block, block)
        write_rows(stage, slot + at, out_hbm, start + at, block, sems.at[sem_at + i]).start()

    def merge_and_send(i):
        merge(i)
        send(i)

    in_groups(size // block, UNROLL, merge_and_send)


def scale_own(gained, scale, stage, slot, out_hbm, start, sems, sem_at):
    size, columns = gained.shape
    block = min(BLOCK, size)
    tile = min(TILE, columns)

    @pl.loop(0, size // block)
    def _(i):
        at = pl.multiple_of(i * block, block)
        for c in range(0, columns, tile):
            value = gained[pl.ds(at, block), c : c + tile].reshape(block // 8, 8, tile)
            scaled = (value * scale[:, c : c + tile][None]).reshape(block, tile)
            stage[pl.ds(slot + at, block), c : c + tile] = scaled.astype(jnp.bfloat16)
        write_rows(stage, slot + at, out_hbm, start + at, block, sems.at[sem_at + i]).start()


def wait_rows(stage, slot, out_hbm, start, size, sems, sem_at):
    block = min(BLOCK, size)

    @pl.loop(0, size // block)
    def _(i):
        at = pl.multiple_of(i * block, block)
        write_rows(stage, slot + at, out_hbm, start + at, block, sems.at[sem_at + i]).wait()


def first_kernel(parts, *refs):
    gained_gate, gained_up, high_gate = refs[:3]
    stats = refs[3 : 3 + parts]
    others = parts - 1
    raws = refs[3 + parts : 3 + parts + others]
    low_gates = refs[3 + parts + others : 3 + parts + 2 * others]
    low_ups = refs[3 + parts + 2 * others : 3 + parts + 3 * others]
    rest = refs[3 + parts + 3 * others :]
    ready_gate, ready_up, column_gate, column_up, low_up_rows, gain_rows, scale_up = rest[:7]
    scale_gate, low_gate_rows, stage, sems = rest[7:]
    rows, columns = gained_gate.shape
    block = min(BLOCK, rows)
    blocks = rows // block
    me = lax.axis_index("fsdp")

    best = stats[0][0:2, :]
    for stat in stats[1:]:
        best = jnp.maximum(best, stat[0:2, :])
    column_gate[...] = best[0:1, :]
    column_up[...] = best[1:2, :]
    scale_gate[...] = jnp.broadcast_to(1.0 / best[0:1, :], (8, columns))
    scale_up[...] = jnp.broadcast_to(1.0 / best[1:2, :], (8, columns))

    start = pl.multiple_of(me * rows, rows)
    scale_own(gained_gate, scale_gate, stage, 0, ready_gate, start, sems, 0)
    for k in range(others):
        spread_rows(low_gates[k][...], stats[k + 1][2:3, :rows], low_gate_rows, gain_rows, k * rows)
        spread_rows(low_ups[k][...], None, low_up_rows, gain_rows, k * rows)
        there = pl.multiple_of(lax.rem(me - (k + 1) + parts, parts) * rows, rows)
        scale_partner(
            raws[k], low_gate_rows, k * rows, gain_rows, k * rows, high_gate, scale_gate,
            stage, (k + 1) * rows, ready_gate, there, sems, (k + 1) * blocks,
        )
    scale_own(gained_up, scale_up, stage, parts * rows, ready_up, start, sems, parts * blocks)
    wait_rows(stage, 0, ready_gate, start, rows, sems, 0)
    for k in range(others):
        there = pl.multiple_of(lax.rem(me - (k + 1) + parts, parts) * rows, rows)
        wait_rows(stage, (k + 1) * rows, ready_gate, there, rows, sems, (k + 1) * blocks)
    wait_rows(stage, parts * rows, ready_up, start, rows, sems, parts * blocks)


def first(gained_gate, gained_up, stats, raws, low_gates, low_ups, high_gate):
    parts = len(stats)
    others = parts - 1
    rows, columns = gained_gate.shape
    rank = high_gate.shape[0]
    blocks = rows // min(BLOCK, rows)
    return pl.pallas_call(
        functools.partial(first_kernel, parts),
        out_shape=(
            pltpu.HBM((parts * rows, columns), jnp.bfloat16),
            pltpu.HBM((parts * rows, columns), jnp.bfloat16),
            jax.ShapeDtypeStruct((1, columns), jnp.float32),
            jax.ShapeDtypeStruct((1, columns), jnp.float32),
            pltpu.VMEM((others * rows, rank), jnp.bfloat16),
            pltpu.VMEM((others * rows, 128), jnp.float32),
            pltpu.VMEM((8, columns), jnp.float32),
        ),
        in_specs=[VMEM_SPEC] * (3 + parts + 3 * others),
        out_specs=(HBM_SPEC, HBM_SPEC) + (VMEM_SPEC,) * 5,
        scratch_shapes=[
            pltpu.VMEM((8, columns), jnp.float32),
            pltpu.VMEM((others * rows, rank), jnp.bfloat16),
            pltpu.VMEM(((parts + 1) * rows, columns), jnp.bfloat16),
            pltpu.SemaphoreType.DMA(((parts + 1) * blocks,)),
        ],
        compiler_params=pltpu.CompilerParams(vmem_limit_bytes=18 * 1024 * 1024),
        cost_estimate=pl.CostEstimate(
            flops=16 * parts * rows * columns * rank, bytes_accessed=4 * parts * rows * columns, transcendentals=0
        ),
    )(
        in_vmem(gained_gate), in_vmem(gained_up), in_vmem(high_gate),
        *map(in_vmem, stats), *map(in_vmem, raws), *map(in_vmem, low_gates), *map(in_vmem, low_ups),
    )


def later_kernel(parts, rows, offset, *refs):
    others = parts - 1
    raws = refs[:others]
    low_rows, gain_rows, scale, high, _, ready, stage, sems = refs[others:]
    size = raws[0].shape[0]
    blocks = size // min(BLOCK, size)
    me = lax.axis_index("fsdp")
    for k in range(others):
        there = pl.multiple_of(lax.rem(me - (k + 1) + parts, parts) * rows + offset, min(BLOCK, size))
        scale_partner(
            raws[k], low_rows, k * rows + offset, gain_rows, k * rows + offset, high, scale,
            stage, k * size, ready, there, sems, k * blocks,
        )
    for k in range(others):
        there = pl.multiple_of(lax.rem(me - (k + 1) + parts, parts) * rows + offset, min(BLOCK, size))
        wait_rows(stage, k * size, ready, there, size, sems, k * blocks)


def later(ready, raws, low_rows, gain_rows, scale, high, rows, offset):
    others = len(raws)
    size, columns = raws[0].shape
    rank = high.shape[0]
    blocks = size // min(BLOCK, size)
    return pl.pallas_call(
        functools.partial(later_kernel, others + 1, rows, offset),
        out_shape=pltpu.HBM(ready.shape, ready.dtype),
        in_specs=[VMEM_SPEC] * (others + 4) + [HBM_SPEC],
        out_specs=HBM_SPEC,
        input_output_aliases={others + 4: 0},
        scratch_shapes=[
            pltpu.VMEM((others * size, columns), jnp.bfloat16),
            pltpu.SemaphoreType.DMA((others * blocks,)),
        ],
        compiler_params=pltpu.CompilerParams(vmem_limit_bytes=8 * 1024 * 1024),
        cost_estimate=pl.CostEstimate(
            flops=16 * others * size * columns * rank, bytes_accessed=4 * others * size * columns, transcendentals=0
        ),
    )(*map(in_vmem, raws), in_vmem(low_rows), in_vmem(gain_rows), in_vmem(scale), in_vmem(high), in_hbm(ready))


def chunks_of(rows):
    block = min(BLOCK, rows)
    blocks = rows // block
    first_size = block * max(1, (blocks + 1) // 2)
    return ((0, first_size), (first_size, rows - first_size)) if first_size < rows else ((0, rows),)


def solution(mesh):
    parts = mesh.shape["fsdp"]

    def around(x):
        return [
            lax.ppermute(x, "fsdp", [(i, (i + k) % parts) for i in range(parts)]) for k in range(1, parts)
        ]

    def per_device(train_gate, low_gate, high_gate, train_up, low_up, high_up, norm_gain):
        rows = train_gate.shape[0]
        chunks = chunks_of(rows)
        gates = around(train_gate)
        low_gates = around(low_gate.T)
        low_ups = around(low_up.T)
        gained_gate, gained_up, stat, high_gate, high_up, *pieces = own(
            train_gate, train_up, low_gate.T, low_up.T, norm_gain.reshape(1, -1), high_gate, high_up, chunks
        )
        stats = [stat] + around(stat)
        ups = [around(piece) for piece in pieces]
        ready_gate, ready_up, column_gate, column_up, low_up_rows, gain_rows, scale_up = first(
            gained_gate, gained_up, stats, gates, low_gates, low_ups, high_gate
        )
        for n, (offset, _) in enumerate(chunks):
            ready_up = later(ready_up, ups[n], low_up_rows, gain_rows, scale_up, high_up, rows, offset)
        return ready_gate, ready_up, column_gate.reshape(-1), column_up.reshape(-1)

    placed = (
        P(("trial", "fsdp"), "cols"),
        P(("trial", "fsdp"), None),
        P("trial", "cols"),
        P(("trial", "fsdp"), "cols"),
        P(("trial", "fsdp"), None),
        P("trial", "cols"),
        P(("trial", "fsdp")),
    )
    return jax.shard_map(
        per_device,
        mesh=mesh,
        in_specs=placed,
        out_specs=(
            P("trial", "cols"),
            P("trial", "cols"),
            P(("trial", "cols")),
            P(("trial", "cols")),
        ),
        check_vma=False,
    )
```

```python
import functools

import jax
import jax.numpy as jnp
from jax import lax
from jax.experimental import pallas as pl
from jax.experimental.pallas import tpu as pltpu
from jax.sharding import PartitionSpec as P


BLOCK = 128
TILE = 256
STAT_ROWS = 8
UNROLL = 4
PRODUCTS = 8


def in_hbm(x):
    return pltpu.with_memory_space_constraint(x, pltpu.HBM)


def in_vmem(x):
    return pltpu.with_memory_space_constraint(x, pltpu.VMEM)


VMEM_SPEC = pl.BlockSpec(memory_space=pltpu.VMEM)
HBM_SPEC = pl.BlockSpec(memory_space=pl.ANY)


def spread_rows(low_t, gain, low_rows, gain_rows, at):
    rows = low_t.shape[1]
    low_rows[at : at + rows, :] = low_t.astype(jnp.float32).T.astype(jnp.bfloat16)
    if gain is not None:
        gain_rows[at : at + rows, :] = jnp.broadcast_to(gain, (128, rows)).T


def multiplied(low_rows, high):
    return lambda at, block, c, tile: jnp.dot(
        low_rows[pl.ds(at, block), :], high[:, c : c + tile], preferred_element_type=jnp.float32
    )


def gained_tile(raw, added, gain):
    latest = raw.astype(jnp.float32) + added
    return latest * jnp.concatenate([gain] * (raw.shape[1] // 128), axis=1)


def in_groups(blocks, limit, *stages):
    def body(first, group):
        for stage in stages:
            for g in range(group):
                stage(first + g)

    @pl.loop(0, blocks // limit)
    def _(n):
        body(n * limit, limit)

    if blocks % limit:
        body(blocks - blocks % limit, blocks % limit)


def own_kernel(chunks, gate_hbm, up_hbm, *refs):
    small_hbm = refs[:5]
    gained_gate, gained_up, stat, high_gate, high_up = refs[5:10]
    pieces = refs[10 : 10 + len(chunks)]
    gate_buf, low_gate_t, low_up_t, gain, low_rows, gain_rows, top, small_sems, gate_sems, up_sems = refs[
        10 + len(chunks) :
    ]
    rows, columns = gate_hbm.shape
    block = min(BLOCK, rows)
    tile = min(TILE, columns)

    def gate_copy(i):
        at = pl.multiple_of(i * block, block)
        return pltpu.make_async_copy(
            gate_hbm.at[pl.ds(at, block), :], gate_buf.at[pl.ds(at, block), :], gate_sems.at[i]
        )

    def up_copy(piece, start, i):
        at = pl.multiple_of(i * block, block)
        return pltpu.make_async_copy(
            up_hbm.at[pl.ds(start + at, block), :], piece.at[pl.ds(at, block), :], up_sems.at[start // block + i]
        )

    small = [
        pltpu.make_async_copy(source, target, small_sems.at[n])
        for n, (source, target) in enumerate(zip(small_hbm, (low_gate_t, low_up_t, gain, high_gate, high_up)))
    ]
    for copy in small:
        copy.start()
    for i in range(rows // block):
        gate_copy(i).start()
    for copy in small:
        copy.wait()
    spread_rows(low_gate_t[...], gain[...], low_rows, gain_rows, 0)
    spread_rows(low_up_t[...], None, low_rows, gain_rows, rows)
    for piece, (start, size) in zip(pieces, chunks):
        for i in range(size // block):
            up_copy(piece, start, i).start()
    top[...] = jnp.zeros_like(top)

    def merge_block(raw_ref, raw_at, start, low_at, high_ref, gained, top_at):
        at = start + raw_at
        adapter = multiplied(low_rows.at[pl.ds(low_at, rows), :], high_ref)
        gain_block = gain_rows[pl.ds(at, block), :]
        for c in range(0, columns, tile):
            value = gained_tile(
                raw_ref[pl.ds(raw_at, block), c : c + tile], adapter(at, block, c, tile), gain_block
            )
            gained[pl.ds(at, block), c : c + tile] = value
            best = jnp.max(jnp.abs(value).reshape(block // 8, 8, tile), axis=0)
            top[top_at : top_at + 8, c : c + tile] = jnp.maximum(top[top_at : top_at + 8, c : c + tile], best)

    in_groups(
        rows // block,
        UNROLL,
        lambda i: gate_copy(i).wait(),
        lambda i: merge_block(gate_buf, pl.multiple_of(i * block, block), 0, 0, high_gate, gained_gate, 0),
    )
    for piece, (start, size) in zip(pieces, chunks):
        in_groups(
            size // block,
            UNROLL,
            lambda i: up_copy(piece, start, i).wait(),
            lambda i: merge_block(piece, pl.multiple_of(i * block, block), start, rows, high_up, gained_up, 8),
        )

    stat[...] = jnp.zeros_like(stat)
    stat[0:1, :] = jnp.max(top[0:8, :], axis=0, keepdims=True)
    stat[1:2, :] = jnp.max(top[8:16, :], axis=0, keepdims=True)
    stat[2:3, :rows] = gain[...]


def own(train_gate, train_up, low_gate_t, low_up_t, gain, high_gate, high_up, chunks):
    rows, columns = train_gate.shape
    rank = high_gate.shape[0]
    block = min(BLOCK, rows)
    return pl.pallas_call(
        functools.partial(own_kernel, chunks),
        out_shape=(
            pltpu.VMEM((rows, columns), jnp.float32),
            pltpu.VMEM((rows, columns), jnp.float32),
            pltpu.VMEM((STAT_ROWS, columns), jnp.float32),
            pltpu.VMEM((rank, columns), jnp.bfloat16),
            pltpu.VMEM((rank, columns), jnp.bfloat16),
            *[pltpu.VMEM((size, columns), jnp.bfloat16) for _, size in chunks],
        ),
        in_specs=[HBM_SPEC] * 7,
        out_specs=(VMEM_SPEC,) * (5 + len(chunks)),
        scratch_shapes=[
            pltpu.VMEM((rows, columns), jnp.bfloat16),
            pltpu.VMEM((rank, rows), jnp.bfloat16),
            pltpu.VMEM((rank, rows), jnp.bfloat16),
            pltpu.VMEM((1, rows), jnp.float32),
            pltpu.VMEM((2 * rows, rank), jnp.bfloat16),
            pltpu.VMEM((rows, 128), jnp.float32),
            pltpu.VMEM((16, columns), jnp.float32),
            pltpu.SemaphoreType.DMA((5,)),
            pltpu.SemaphoreType.DMA((rows // block,)),
            pltpu.SemaphoreType.DMA((rows // block,)),
        ],
        compiler_params=pltpu.CompilerParams(vmem_limit_bytes=12 * 1024 * 1024),
        cost_estimate=pl.CostEstimate(
            flops=32 * rows * columns * rank, bytes_accessed=4 * rows * columns, transcendentals=0
        ),
    )(*map(in_hbm, (train_gate, train_up, low_gate_t, low_up_t, gain, high_gate, high_up)))


def write_rows(stage, slot, out_hbm, start, size, sem):
    return pltpu.make_async_copy(stage.at[pl.ds(slot, size), :], out_hbm.at[pl.ds(start, size), :], sem)


def scale_partner(raw, adapter, gain_rows, gain_at, scale, stage, slot, out_hbm, start, sems, sem_at):
    size, columns = raw.shape
    block = min(BLOCK, size)
    tile = min(TILE, columns)

    def merge(i):
        at = pl.multiple_of(i * block, block)
        gain_block = gain_rows[pl.ds(gain_at + at, block), :]
        for c in range(0, columns, tile):
            value = gained_tile(raw[pl.ds(at, block), c : c + tile], adapter(at, block, c, tile), gain_block)
            scaled = value.reshape(block // 8, 8, tile) * scale[:, c : c + tile][None]
            stage[pl.ds(slot + at, block), c : c + tile] = scaled.reshape(block, tile).astype(jnp.bfloat16)

    def send(i):
        at = pl.multiple_of(i * block, block)
        write_rows(stage, slot + at, out_hbm, start + at, block, sems.at[sem_at + i]).start()

    def merge_and_send(i):
        merge(i)
        send(i)

    in_groups(size // block, UNROLL, merge_and_send)


def scale_own(gained, scale, stage, slot, out_hbm, start, sems, sem_at):
    size, columns = gained.shape
    block = min(BLOCK, size)
    tile = min(TILE, columns)

    @pl.loop(0, size // block)
    def _(i):
        at = pl.multiple_of(i * block, block)
        for c in range(0, columns, tile):
            value = gained[pl.ds(at, block), c : c + tile].reshape(block // 8, 8, tile)
            scaled = (value * scale[:, c : c + tile][None]).reshape(block, tile)
            stage[pl.ds(slot + at, block), c : c + tile] = scaled.astype(jnp.bfloat16)
        write_rows(stage, slot + at, out_hbm, start + at, block, sems.at[sem_at + i]).start()


def wait_rows(stage, slot, out_hbm, start, size, sems, sem_at):
    block = min(BLOCK, size)

    @pl.loop(0, size // block)
    def _(i):
        at = pl.multiple_of(i * block, block)
        write_rows(stage, slot + at, out_hbm, start + at, block, sems.at[sem_at + i]).wait()


def first_kernel(parts, *refs):
    gained_gate, gained_up, high_gate, high_up = refs[:4]
    stats = refs[4 : 4 + parts]
    others = parts - 1
    raws = refs[4 + parts : 4 + parts + others]
    low_gates = refs[4 + parts + others : 4 + parts + 2 * others]
    low_ups = refs[4 + parts + 2 * others : 4 + parts + 3 * others]
    rest = refs[4 + parts + 3 * others :]
    ready_gate, ready_up, column_gate, column_up, product_up, gain_rows, scale_up = rest[:7]
    scale_gate, low_gate_rows, low_up_rows, stage, sems = rest[7:]
    rows, columns = gained_gate.shape
    block = min(BLOCK, rows)
    blocks = rows // block
    tile = min(TILE, columns)
    me = lax.axis_index("fsdp")

    best = stats[0][0:2, :]
    for stat in stats[1:]:
        best = jnp.maximum(best, stat[0:2, :])
    column_gate[...] = best[0:1, :]
    column_up[...] = best[1:2, :]
    scale_gate[...] = jnp.broadcast_to(1.0 / best[0:1, :], (8, columns))
    scale_up[...] = jnp.broadcast_to(1.0 / best[1:2, :], (8, columns))

    start = pl.multiple_of(me * rows, rows)
    scale_own(gained_gate, scale_gate, stage, 0, ready_gate, start, sems, 0)
    for k in range(others):
        spread_rows(low_gates[k][...], stats[k + 1][2:3, :rows], low_gate_rows, gain_rows, k * rows)
        spread_rows(low_ups[k][...], None, low_up_rows, gain_rows, k * rows)
        there = pl.multiple_of(lax.rem(me - (k + 1) + parts, parts) * rows, rows)
        scale_partner(
            raws[k], multiplied(low_gate_rows.at[pl.ds(k * rows, rows), :], high_gate), gain_rows, k * rows, scale_gate,
            stage, (k + 1) * rows, ready_gate, there, sems, (k + 1) * blocks,
        )
    scale_own(gained_up, scale_up, stage, parts * rows, ready_up, start, sems, parts * blocks)

    def product(n):
        c = pl.multiple_of(n * tile, tile)
        product_up[:, pl.ds(c, tile)] = jnp.dot(
            low_up_rows[...], high_up[:, pl.ds(c, tile)], preferred_element_type=jnp.float32
        )

    in_groups(columns // tile, PRODUCTS, product)
    wait_rows(stage, 0, ready_gate, start, rows, sems, 0)
    for k in range(others):
        there = pl.multiple_of(lax.rem(me - (k + 1) + parts, parts) * rows, rows)
        wait_rows(stage, (k + 1) * rows, ready_gate, there, rows, sems, (k + 1) * blocks)
    wait_rows(stage, parts * rows, ready_up, start, rows, sems, parts * blocks)


def first(gained_gate, gained_up, stats, raws, low_gates, low_ups, high_gate, high_up):
    parts = len(stats)
    others = parts - 1
    rows, columns = gained_gate.shape
    rank = high_gate.shape[0]
    blocks = rows // min(BLOCK, rows)
    return pl.pallas_call(
        functools.partial(first_kernel, parts),
        out_shape=(
            pltpu.HBM((parts * rows, columns), jnp.bfloat16),
            pltpu.HBM((parts * rows, columns), jnp.bfloat16),
            jax.ShapeDtypeStruct((1, columns), jnp.float32),
            jax.ShapeDtypeStruct((1, columns), jnp.float32),
            pltpu.VMEM((others * rows, columns), jnp.float32),
            pltpu.VMEM((others * rows, 128), jnp.float32),
            pltpu.VMEM((8, columns), jnp.float32),
        ),
        in_specs=[VMEM_SPEC] * (4 + parts + 3 * others),
        out_specs=(HBM_SPEC, HBM_SPEC) + (VMEM_SPEC,) * 5,
        scratch_shapes=[
            pltpu.VMEM((8, columns), jnp.float32),
            pltpu.VMEM((others * rows, rank), jnp.bfloat16),
            pltpu.VMEM((others * rows, rank), jnp.bfloat16),
            pltpu.VMEM(((parts + 1) * rows, columns), jnp.bfloat16),
            pltpu.SemaphoreType.DMA(((parts + 1) * blocks,)),
        ],
        compiler_params=pltpu.CompilerParams(vmem_limit_bytes=18 * 1024 * 1024),
        cost_estimate=pl.CostEstimate(
            flops=16 * parts * rows * columns * rank, bytes_accessed=4 * parts * rows * columns, transcendentals=0
        ),
    )(
        in_vmem(gained_gate), in_vmem(gained_up), in_vmem(high_gate), in_vmem(high_up),
        *map(in_vmem, stats), *map(in_vmem, raws), *map(in_vmem, low_gates), *map(in_vmem, low_ups),
    )


def later_kernel(parts, rows, offset, *refs):
    others = parts - 1
    raws = refs[:others]
    product, gain_rows, scale, _, ready, stage, sems = refs[others:]
    size = raws[0].shape[0]
    blocks = size // min(BLOCK, size)
    me = lax.axis_index("fsdp")
    for k in range(others):
        there = pl.multiple_of(lax.rem(me - (k + 1) + parts, parts) * rows + offset, min(BLOCK, size))

        def added(at, block, c, tile, k=k):
            return product[pl.ds(k * rows + offset + at, block), c : c + tile]

        scale_partner(
            raws[k], added, gain_rows, k * rows + offset, scale,
            stage, k * size, ready, there, sems, k * blocks,
        )
    for k in range(others):
        there = pl.multiple_of(lax.rem(me - (k + 1) + parts, parts) * rows + offset, min(BLOCK, size))
        wait_rows(stage, k * size, ready, there, size, sems, k * blocks)


def later(ready, raws, product, gain_rows, scale, rows, offset):
    others = len(raws)
    size, columns = raws[0].shape
    blocks = size // min(BLOCK, size)
    return pl.pallas_call(
        functools.partial(later_kernel, others + 1, rows, offset),
        out_shape=pltpu.HBM(ready.shape, ready.dtype),
        in_specs=[VMEM_SPEC] * (others + 3) + [HBM_SPEC],
        out_specs=HBM_SPEC,
        input_output_aliases={others + 3: 0},
        scratch_shapes=[
            pltpu.VMEM((others * size, columns), jnp.bfloat16),
            pltpu.SemaphoreType.DMA((others * blocks,)),
        ],
        compiler_params=pltpu.CompilerParams(vmem_limit_bytes=8 * 1024 * 1024),
        cost_estimate=pl.CostEstimate(
            flops=256 * others * size * columns, bytes_accessed=4 * others * size * columns, transcendentals=0
        ),
    )(*map(in_vmem, raws), in_vmem(product), in_vmem(gain_rows), in_vmem(scale), in_hbm(ready))


def chunks_of(rows):
    return ((0, rows),)


def solution(mesh):
    parts = mesh.shape["fsdp"]

    def around(x):
        return [
            lax.ppermute(x, "fsdp", [(i, (i + k) % parts) for i in range(parts)]) for k in range(1, parts)
        ]

    def per_device(train_gate, low_gate, high_gate, train_up, low_up, high_up, norm_gain):
        rows = train_gate.shape[0]
        chunks = chunks_of(rows)
        gates = around(train_gate)
        low_gates = around(low_gate.T)
        low_ups = around(low_up.T)
        gained_gate, gained_up, stat, high_gate, high_up, *pieces = own(
            train_gate, train_up, low_gate.T, low_up.T, norm_gain.reshape(1, -1), high_gate, high_up, chunks
        )
        stats = [stat] + around(stat)
        ups = [around(piece) for piece in pieces]
        ready_gate, ready_up, column_gate, column_up, product_up, gain_rows, scale_up = first(
            gained_gate, gained_up, stats, gates, low_gates, low_ups, high_gate, high_up
        )
        for n, (offset, _) in enumerate(chunks):
            ready_up = later(ready_up, ups[n], product_up, gain_rows, scale_up, rows, offset)
        return ready_gate, ready_up, column_gate.reshape(-1), column_up.reshape(-1)

    placed = (
        P(("trial", "fsdp"), "cols"),
        P(("trial", "fsdp"), None),
        P("trial", "cols"),
        P(("trial", "fsdp"), "cols"),
        P(("trial", "fsdp"), None),
        P("trial", "cols"),
        P(("trial", "fsdp")),
    )
    return jax.shard_map(
        per_device,
        mesh=mesh,
        in_specs=placed,
        out_specs=(
            P("trial", "cols"),
            P("trial", "cols"),
            P(("trial", "cols")),
            P(("trial", "cols")),
        ),
        check_vma=False,
    )
```

```python
import functools

import jax
import jax.numpy as jnp
from jax import lax
from jax.experimental import pallas as pl
from jax.experimental.pallas import tpu as pltpu
from jax.sharding import PartitionSpec as P


BLOCK = 128
TILE = 256
UNROLL = 4
PRODUCTS = 8
LATER_UNROLL = 1
LATER_BLOCK = 64
PART = 64
EARLY = 64


def in_hbm(x):
    return pltpu.with_memory_space_constraint(x, pltpu.HBM)


def in_vmem(x):
    return pltpu.with_memory_space_constraint(x, pltpu.VMEM)


VMEM_SPEC = pl.BlockSpec(memory_space=pltpu.VMEM)
HBM_SPEC = pl.BlockSpec(memory_space=pl.ANY)


def spread_rows(low_t, gain, low_rows, gain_rows, at):
    rows = low_t.shape[1]
    low_rows[at : at + rows, :] = low_t.astype(jnp.float32).T.astype(jnp.bfloat16)
    if gain is not None:
        gain_rows[at : at + rows, :] = jnp.broadcast_to(gain, (128, rows)).T


def multiplied(low_rows, high):
    return lambda at, block, c, tile: jnp.dot(
        low_rows[pl.ds(at, block), :], high[:, c : c + tile], preferred_element_type=jnp.float32
    )


def gained_tile(raw, added, gain):
    latest = raw.astype(jnp.float32) + added
    return latest * jnp.concatenate([gain] * (raw.shape[1] // 128), axis=1)


def in_groups(blocks, limit, *stages):
    def body(first, group):
        for stage in stages:
            for g in range(group):
                stage(first + g)

    @pl.loop(0, blocks // limit)
    def _(n):
        body(n * limit, limit)

    if blocks % limit:
        body(blocks - blocks % limit, blocks % limit)


def own_kernel(chunks, gate_hbm, up_hbm, *refs):
    small_hbm = refs[:5]
    gained_gate, gained_up, news, lows, high_gate, high_up = refs[5:11]
    rank = high_gate.shape[0]
    pieces = [refs[11]]
    if len(chunks) > 1:
        pieces.append(lows.at[pl.ds(rank, chunks[1][1]), :])
    gate_buf, low_gate_t, low_up_t, gain, low_rows, gain_rows, top, small_sems, gate_sems, up_sems = refs[12:]
    rows, columns = gate_hbm.shape
    block = min(BLOCK, rows)
    tile = min(TILE, columns)

    def gate_copy(i):
        at = pl.multiple_of(i * block, block)
        return pltpu.make_async_copy(
            gate_hbm.at[pl.ds(at, block), :], gate_buf.at[pl.ds(at, block), :], gate_sems.at[i]
        )

    def up_copy(piece, start, i, count=block):
        at = pl.multiple_of(i * block, block)
        sem = up_sems.at[start // PART + i * (block // PART)]
        return pltpu.make_async_copy(
            up_hbm.at[pl.ds(start + at, count), :], piece.at[pl.ds(at, count), :], sem
        )

    small = [
        pltpu.make_async_copy(source, target, small_sems.at[n])
        for n, (source, target) in enumerate(zip(small_hbm, (low_gate_t, low_up_t, gain, high_gate, high_up)))
    ]
    for copy in small:
        copy.start()
    for i in range(rows // block):
        gate_copy(i).start()
    for copy in small:
        copy.wait()
    spread_rows(low_gate_t[...], gain[...], low_rows, gain_rows, 0)
    spread_rows(low_up_t[...], None, low_rows, gain_rows, rows)
    for piece, (start, size) in zip(pieces, chunks):
        for i in range(size // block):
            up_copy(piece, start, i).start()
        if size % block:
            up_copy(piece, start, size // block, size % block).start()
    top[...] = jnp.zeros_like(top)

    def merge_block(raw_ref, raw_at, start, low_at, high_ref, gained, top_at, block=block):
        at = start + raw_at
        adapter = multiplied(low_rows.at[pl.ds(low_at, rows), :], high_ref)
        gain_block = gain_rows[pl.ds(at, block), :]
        for c in range(0, columns, tile):
            value = gained_tile(
                raw_ref[pl.ds(raw_at, block), c : c + tile], adapter(at, block, c, tile), gain_block
            )
            gained[pl.ds(at, block), c : c + tile] = value
            best = jnp.max(jnp.abs(value).reshape(block // 8, 8, tile), axis=0)
            top[top_at : top_at + 8, c : c + tile] = jnp.maximum(top[top_at : top_at + 8, c : c + tile], best)

    in_groups(
        rows // block,
        UNROLL,
        lambda i: gate_copy(i).wait(),
        lambda i: merge_block(gate_buf, pl.multiple_of(i * block, block), 0, 0, high_gate, gained_gate, 0),
    )
    for piece, (start, size) in zip(pieces, chunks):
        in_groups(
            size // block,
            UNROLL,
            lambda i: up_copy(piece, start, i).wait(),
            lambda i: merge_block(piece, pl.multiple_of(i * block, block), start, rows, high_up, gained_up, 8),
        )
        if size % block:
            up_copy(piece, start, size // block, size % block).wait()
            merge_block(piece, size - size % block, start, rows, high_up, gained_up, 8, size % block)

    news[:, :columns] = jnp.max(top[0:8, :], axis=0, keepdims=True)
    news[:, columns : 2 * columns] = jnp.max(top[8:16, :], axis=0, keepdims=True)
    news[:, 2 * columns :] = gain[...]
    lows[:rank, :rows] = low_gate_t[...]
    lows[:rank, rows : 2 * rows] = low_up_t[...]


def own(train_gate, train_up, low_gate_t, low_up_t, gain, high_gate, high_up, chunks):
    rows, columns = train_gate.shape
    rank = high_gate.shape[0]
    block = min(BLOCK, rows)
    return pl.pallas_call(
        functools.partial(own_kernel, chunks),
        out_shape=(
            pltpu.VMEM((rows, columns), jnp.float32),
            pltpu.VMEM((rows, columns), jnp.float32),
            pltpu.VMEM((1, 2 * columns + rows), jnp.float32),
            pltpu.VMEM((rank + rows - chunks[0][1], max(columns, 2 * rows)), jnp.bfloat16),
            pltpu.VMEM((rank, columns), jnp.bfloat16),
            pltpu.VMEM((rank, columns), jnp.bfloat16),
            pltpu.VMEM((chunks[0][1], columns), jnp.bfloat16),
        ),
        in_specs=[HBM_SPEC] * 7,
        out_specs=(VMEM_SPEC,) * 7,
        scratch_shapes=[
            pltpu.VMEM((rows, columns), jnp.bfloat16),
            pltpu.VMEM((rank, rows), jnp.bfloat16),
            pltpu.VMEM((rank, rows), jnp.bfloat16),
            pltpu.VMEM((1, rows), jnp.float32),
            pltpu.VMEM((2 * rows, rank), jnp.bfloat16),
            pltpu.VMEM((rows, 128), jnp.float32),
            pltpu.VMEM((16, columns), jnp.float32),
            pltpu.SemaphoreType.DMA((5,)),
            pltpu.SemaphoreType.DMA((rows // block,)),
            pltpu.SemaphoreType.DMA((rows // PART,)),
        ],
        compiler_params=pltpu.CompilerParams(vmem_limit_bytes=12 * 1024 * 1024),
        cost_estimate=pl.CostEstimate(
            flops=32 * rows * columns * rank, bytes_accessed=4 * rows * columns, transcendentals=0
        ),
    )(*map(in_hbm, (train_gate, train_up, low_gate_t, low_up_t, gain, high_gate, high_up)))


def write_rows(stage, slot, out_hbm, start, size, sem):
    return pltpu.make_async_copy(stage.at[pl.ds(slot, size), :], out_hbm.at[pl.ds(start, size), :], sem)


def scale_partner(
    raw, adapter, gain_rows, gain_at, scale, stage, slot, out_hbm, start, sems, sem_at, group=UNROLL, block=BLOCK
):
    size, columns = raw.shape
    block = min(block, size)
    tile = min(TILE, columns)

    def merge(i):
        at = pl.multiple_of(i * block, block)
        gain_block = gain_rows[pl.ds(gain_at + at, block), :]
        for c in range(0, columns, tile):
            value = gained_tile(raw[pl.ds(at, block), c : c + tile], adapter(at, block, c, tile), gain_block)
            scaled = value.reshape(block // 8, 8, tile) * scale[:, c : c + tile][None]
            stage[pl.ds(slot + at, block), c : c + tile] = scaled.reshape(block, tile).astype(jnp.bfloat16)

    def send(i):
        at = pl.multiple_of(i * block, block)
        write_rows(stage, slot + at, out_hbm, start + at, block, sems.at[sem_at + i]).start()

    def merge_and_send(i):
        merge(i)
        send(i)

    in_groups(size // block, group, merge_and_send)


def scale_own(gained, scale, stage, slot, out_hbm, start, sems, sem_at):
    size, columns = gained.shape
    block = min(BLOCK, size)
    tile = min(TILE, columns)

    @pl.loop(0, size // block)
    def _(i):
        at = pl.multiple_of(i * block, block)
        for c in range(0, columns, tile):
            value = gained[pl.ds(at, block), c : c + tile].reshape(block // 8, 8, tile)
            scaled = (value * scale[:, c : c + tile][None]).reshape(block, tile)
            stage[pl.ds(slot + at, block), c : c + tile] = scaled.astype(jnp.bfloat16)
        write_rows(stage, slot + at, out_hbm, start + at, block, sems.at[sem_at + i]).start()


def wait_rows(stage, slot, out_hbm, start, size, sems, sem_at, block=BLOCK):
    block = min(block, size)

    @pl.loop(0, size // block)
    def _(i):
        at = pl.multiple_of(i * block, block)
        write_rows(stage, slot + at, out_hbm, start + at, block, sems.at[sem_at + i]).wait()


def first_kernel(parts, offset, *refs):
    gained_gate, gained_up, high_gate, high_up = refs[:4]
    news = refs[4 : 4 + parts]
    others = parts - 1
    raws = refs[4 + parts : 4 + parts + others]
    lows = refs[4 + parts + others : 4 + parts + 2 * others]
    rank = high_gate.shape[0]
    early = [low.at[pl.ds(rank, low.shape[0] - rank), :] for low in lows] if lows[0].shape[0] > rank else []
    rest = refs[len(refs) - 12 :]
    ready_gate, ready_up, column_gate, column_up, product_up, gain_rows, scale_up = rest[:7]
    scale_gate, low_gate_rows, low_up_rows, stage, sems = rest[7:]
    rows, columns = gained_gate.shape
    block = min(BLOCK, rows)
    blocks = rows // block
    tile = min(TILE, columns)
    me = lax.axis_index("fsdp")

    for at, column, scale in ((0, column_gate, scale_gate), (columns, column_up, scale_up)):
        best = news[0][:, at : at + columns]
        for new in news[1:]:
            best = jnp.maximum(best, new[:, at : at + columns])
        column[...] = best
        scale[...] = jnp.broadcast_to(1.0 / best, (8, columns))

    start = pl.multiple_of(me * rows, rows)
    scale_own(gained_gate, scale_gate, stage, 0, ready_gate, start, sems, 0)
    scale_own(gained_up, scale_up, stage, parts * rows, ready_up, start, sems, parts * blocks)
    for k in range(others):
        spread_rows(lows[k][:rank, :rows], news[k + 1][:, 2 * columns :], low_gate_rows, gain_rows, k * rows)
        spread_rows(lows[k][:rank, rows : 2 * rows], None, low_up_rows, gain_rows, k * rows)
        there = pl.multiple_of(lax.rem(me - (k + 1) + parts, parts) * rows, rows)
        scale_partner(
            raws[k], multiplied(low_gate_rows.at[pl.ds(k * rows, rows), :], high_gate), gain_rows, k * rows, scale_gate,
            stage, (k + 1) * rows, ready_gate, there, sems, (k + 1) * blocks,
        )

    def early_rows(k):
        size = early[k].shape[0]
        there = pl.multiple_of(lax.rem(me - (k + 1) + parts, parts) * rows + offset, size)
        return size, (parts + 1) * rows + k * size, there, (parts + 1) * blocks + k

    for k in range(len(early)):
        size, slot, there, sem_at = early_rows(k)
        scale_partner(
            early[k], multiplied(low_up_rows.at[pl.ds(k * rows + offset, size), :], high_up),
            gain_rows, k * rows + offset, scale_up, stage, slot, ready_up, there, sems, sem_at, 1, size,
        )

    def product(n):
        c = pl.multiple_of(n * tile, tile)
        product_up[:, pl.ds(c, tile)] = jnp.dot(
            low_up_rows[...], high_up[:, pl.ds(c, tile)], preferred_element_type=jnp.float32
        )

    in_groups(columns // tile, PRODUCTS, product)

    for k in range(len(early)):
        size, slot, there, sem_at = early_rows(k)
        wait_rows(stage, slot, ready_up, there, size, sems, sem_at, size)
    wait_rows(stage, 0, ready_gate, start, rows, sems, 0)
    for k in range(others):
        there = pl.multiple_of(lax.rem(me - (k + 1) + parts, parts) * rows, rows)
        wait_rows(stage, (k + 1) * rows, ready_gate, there, rows, sems, (k + 1) * blocks)
    wait_rows(stage, parts * rows, ready_up, start, rows, sems, parts * blocks)


def first(gained_gate, gained_up, news, raws, lows, offset, high_gate, high_up):
    parts = len(news)
    others = parts - 1
    rows, columns = gained_gate.shape
    rank = high_gate.shape[0]
    early = others * (lows[0].shape[0] - rank)
    blocks = rows // min(BLOCK, rows)
    return pl.pallas_call(
        functools.partial(first_kernel, parts, offset),
        out_shape=(
            pltpu.HBM((parts * rows, columns), jnp.bfloat16),
            pltpu.HBM((parts * rows, columns), jnp.bfloat16),
            jax.ShapeDtypeStruct((1, columns), jnp.float32),
            jax.ShapeDtypeStruct((1, columns), jnp.float32),
            pltpu.VMEM((others * rows, columns), jnp.float32),
            pltpu.VMEM((others * rows, 128), jnp.float32),
            pltpu.VMEM((8, columns), jnp.float32),
        ),
        in_specs=[VMEM_SPEC] * (4 + parts + 2 * others),
        out_specs=(HBM_SPEC, HBM_SPEC) + (VMEM_SPEC,) * 5,
        scratch_shapes=[
            pltpu.VMEM((8, columns), jnp.float32),
            pltpu.VMEM((others * rows, rank), jnp.bfloat16),
            pltpu.VMEM((others * rows, rank), jnp.bfloat16),
            pltpu.VMEM(((parts + 1) * rows + early, columns), jnp.bfloat16),
            pltpu.SemaphoreType.DMA(((parts + 1) * blocks + others,)),
        ],
        compiler_params=pltpu.CompilerParams(vmem_limit_bytes=19 * 1024 * 1024),
        cost_estimate=pl.CostEstimate(
            flops=16 * parts * rows * columns * rank, bytes_accessed=4 * parts * rows * columns, transcendentals=0
        ),
    )(
        in_vmem(gained_gate), in_vmem(gained_up), in_vmem(high_gate), in_vmem(high_up),
        *map(in_vmem, news), *map(in_vmem, raws), *map(in_vmem, lows),
    )


def later_kernel(parts, rows, offset, *refs):
    others = parts - 1
    raws = refs[:others]
    product, gain_rows, scale, _, ready, stage, sems = refs[others:]
    size = raws[0].shape[0]
    blocks = size // min(LATER_BLOCK, size)
    me = lax.axis_index("fsdp")
    for k in range(others):
        there = pl.multiple_of(lax.rem(me - (k + 1) + parts, parts) * rows + offset, min(LATER_BLOCK, size))

        def added(at, block, c, tile, k=k):
            return product[pl.ds(k * rows + offset + at, block), c : c + tile]

        scale_partner(
            raws[k], added, gain_rows, k * rows + offset, scale,
            stage, k * size, ready, there, sems, k * blocks, LATER_UNROLL, LATER_BLOCK,
        )
    for k in range(others):
        there = pl.multiple_of(lax.rem(me - (k + 1) + parts, parts) * rows + offset, min(LATER_BLOCK, size))
        wait_rows(stage, k * size, ready, there, size, sems, k * blocks, LATER_BLOCK)


def later(ready, raws, product, gain_rows, scale, rows, offset):
    others = len(raws)
    size, columns = raws[0].shape
    blocks = size // min(LATER_BLOCK, size)
    return pl.pallas_call(
        functools.partial(later_kernel, others + 1, rows, offset),
        out_shape=pltpu.HBM(ready.shape, ready.dtype),
        in_specs=[VMEM_SPEC] * (others + 3) + [HBM_SPEC],
        out_specs=HBM_SPEC,
        input_output_aliases={others + 3: 0},
        scratch_shapes=[
            pltpu.VMEM((others * size, columns), jnp.bfloat16),
            pltpu.SemaphoreType.DMA((others * blocks,)),
        ],
        compiler_params=pltpu.CompilerParams(vmem_limit_bytes=8 * 1024 * 1024),
        cost_estimate=pl.CostEstimate(
            flops=256 * others * size * columns, bytes_accessed=4 * others * size * columns, transcendentals=0
        ),
    )(*map(in_vmem, raws), in_vmem(product), in_vmem(gain_rows), in_vmem(scale), in_hbm(ready))


def chunks_of(rows, columns):
    early = EARLY if rows >= 8 * EARLY and 2 * rows == columns else 0
    return ((0, rows - early),) + (((rows - early, early),) if early else ())


def solution(mesh):
    parts = mesh.shape["fsdp"]

    def around(x):
        return [
            lax.ppermute(x, "fsdp", [(i, (i + k) % parts) for i in range(parts)]) for k in range(1, parts)
        ]

    def per_device(train_gate, low_gate, high_gate, train_up, low_up, high_up, norm_gain):
        rows = train_gate.shape[0]
        chunks = chunks_of(*train_gate.shape)
        gates = around(train_gate)
        gained_gate, gained_up, new, low, high_gate, high_up, piece = own(
            train_gate, train_up, low_gate.T, low_up.T, norm_gain.reshape(1, -1), high_gate, high_up, chunks
        )
        news = [new] + around(new)
        lows = around(low)
        ups = around(piece)
        ready_gate, ready_up, column_gate, column_up, product_up, gain_rows, scale_up = first(
            gained_gate, gained_up, news, gates, lows, chunks[-1][0], high_gate, high_up
        )
        ready_up = later(ready_up, ups, product_up, gain_rows, scale_up, rows, 0)
        return ready_gate, ready_up, column_gate.reshape(-1), column_up.reshape(-1)

    placed = (
        P(("trial", "fsdp"), "cols"),
        P(("trial", "fsdp"), None),
        P("trial", "cols"),
        P(("trial", "fsdp"), "cols"),
        P(("trial", "fsdp"), None),
        P("trial", "cols"),
        P(("trial", "fsdp")),
    )
    return jax.shard_map(
        per_device,
        mesh=mesh,
        in_specs=placed,
        out_specs=(
            P("trial", "cols"),
            P("trial", "cols"),
            P(("trial", "cols")),
            P(("trial", "cols")),
        ),
        check_vma=False,
    )
```

```python
import functools

import jax
import jax.numpy as jnp
from jax import lax
from jax.experimental import pallas as pl
from jax.experimental.pallas import tpu as pltpu
from jax.sharding import PartitionSpec as P


BLOCK = 128
TILE = 256
UNROLL = 4
PRODUCTS = 8
LATER_UNROLL = 1
LATER_BLOCK = 64


def in_hbm(x):
    return pltpu.with_memory_space_constraint(x, pltpu.HBM)


def in_vmem(x):
    return pltpu.with_memory_space_constraint(x, pltpu.VMEM)


VMEM_SPEC = pl.BlockSpec(memory_space=pltpu.VMEM)
HBM_SPEC = pl.BlockSpec(memory_space=pl.ANY)


def spread_rows(low_t, gain, low_rows, gain_rows, at):
    rows = low_t.shape[1]
    low_rows[at : at + rows, :] = low_t.astype(jnp.float32).T.astype(jnp.bfloat16)
    if gain is not None:
        gain_rows[at : at + rows, :] = jnp.broadcast_to(gain, (128, rows)).T


def multiplied(low_rows, high):
    return lambda at, block, c, tile: jnp.dot(
        low_rows[pl.ds(at, block), :], high[:, c : c + tile], preferred_element_type=jnp.float32
    )


def gained_tile(raw, added, gain):
    latest = raw.astype(jnp.float32) + added
    return latest * jnp.concatenate([gain] * (raw.shape[1] // 128), axis=1)


def in_groups(blocks, limit, *stages):
    def body(first, group):
        for stage in stages:
            for g in range(group):
                stage(first + g)

    @pl.loop(0, blocks // limit)
    def _(n):
        body(n * limit, limit)

    if blocks % limit:
        body(blocks - blocks % limit, blocks % limit)


def own_kernel(chunks, gate_hbm, up_hbm, *refs):
    small_hbm = refs[:5]
    gained_gate, gained_up, news, lows, high_gate, high_up = refs[5:11]
    pieces = refs[11 : 11 + len(chunks)]
    gate_buf, low_gate_t, low_up_t, gain, low_rows, gain_rows, top, small_sems, gate_sems, up_sems = refs[
        11 + len(chunks) :
    ]
    rows, columns = gate_hbm.shape
    block = min(BLOCK, rows)
    tile = min(TILE, columns)

    def gate_copy(i):
        at = pl.multiple_of(i * block, block)
        return pltpu.make_async_copy(
            gate_hbm.at[pl.ds(at, block), :], gate_buf.at[pl.ds(at, block), :], gate_sems.at[i]
        )

    def up_copy(piece, start, i):
        at = pl.multiple_of(i * block, block)
        return pltpu.make_async_copy(
            up_hbm.at[pl.ds(start + at, block), :], piece.at[pl.ds(at, block), :], up_sems.at[start // block + i]
        )

    small = [
        pltpu.make_async_copy(source, target, small_sems.at[n])
        for n, (source, target) in enumerate(zip(small_hbm, (low_gate_t, low_up_t, gain, high_gate, high_up)))
    ]
    for copy in small:
        copy.start()
    for i in range(rows // block):
        gate_copy(i).start()
    for copy in small:
        copy.wait()
    spread_rows(low_gate_t[...], gain[...], low_rows, gain_rows, 0)
    spread_rows(low_up_t[...], None, low_rows, gain_rows, rows)
    for piece, (start, size) in zip(pieces, chunks):
        for i in range(size // block):
            up_copy(piece, start, i).start()
    top[...] = jnp.zeros_like(top)

    def merge_block(raw_ref, raw_at, start, low_at, high_ref, gained, top_at):
        at = start + raw_at
        adapter = multiplied(low_rows.at[pl.ds(low_at, rows), :], high_ref)
        gain_block = gain_rows[pl.ds(at, block), :]
        for c in range(0, columns, tile):
            value = gained_tile(
                raw_ref[pl.ds(raw_at, block), c : c + tile], adapter(at, block, c, tile), gain_block
            )
            gained[pl.ds(at, block), c : c + tile] = value
            best = jnp.max(jnp.abs(value).reshape(block // 8, 8, tile), axis=0)
            top[top_at : top_at + 8, c : c + tile] = jnp.maximum(top[top_at : top_at + 8, c : c + tile], best)

    in_groups(
        rows // block,
        UNROLL,
        lambda i: gate_copy(i).wait(),
        lambda i: merge_block(gate_buf, pl.multiple_of(i * block, block), 0, 0, high_gate, gained_gate, 0),
    )
    for piece, (start, size) in zip(pieces, chunks):
        in_groups(
            size // block,
            UNROLL,
            lambda i: up_copy(piece, start, i).wait(),
            lambda i: merge_block(piece, pl.multiple_of(i * block, block), start, rows, high_up, gained_up, 8),
        )

    news[:, :columns] = jnp.max(top[0:8, :], axis=0, keepdims=True)
    news[:, columns : 2 * columns] = jnp.max(top[8:16, :], axis=0, keepdims=True)
    news[:, 2 * columns :] = gain[...]
    lows[:, :rows] = low_gate_t[...]
    lows[:, rows:] = low_up_t[...]


def own(train_gate, train_up, low_gate_t, low_up_t, gain, high_gate, high_up, chunks):
    rows, columns = train_gate.shape
    rank = high_gate.shape[0]
    block = min(BLOCK, rows)
    return pl.pallas_call(
        functools.partial(own_kernel, chunks),
        out_shape=(
            pltpu.VMEM((rows, columns), jnp.float32),
            pltpu.VMEM((rows, columns), jnp.float32),
            pltpu.VMEM((1, 2 * columns + rows), jnp.float32),
            pltpu.VMEM((rank, 2 * rows), jnp.bfloat16),
            pltpu.VMEM((rank, columns), jnp.bfloat16),
            pltpu.VMEM((rank, columns), jnp.bfloat16),
            *[pltpu.VMEM((size, columns), jnp.bfloat16) for _, size in chunks],
        ),
        in_specs=[HBM_SPEC] * 7,
        out_specs=(VMEM_SPEC,) * (6 + len(chunks)),
        scratch_shapes=[
            pltpu.VMEM((rows, columns), jnp.bfloat16),
            pltpu.VMEM((rank, rows), jnp.bfloat16),
            pltpu.VMEM((rank, rows), jnp.bfloat16),
            pltpu.VMEM((1, rows), jnp.float32),
            pltpu.VMEM((2 * rows, rank), jnp.bfloat16),
            pltpu.VMEM((rows, 128), jnp.float32),
            pltpu.VMEM((16, columns), jnp.float32),
            pltpu.SemaphoreType.DMA((5,)),
            pltpu.SemaphoreType.DMA((rows // block,)),
            pltpu.SemaphoreType.DMA((rows // block,)),
        ],
        compiler_params=pltpu.CompilerParams(vmem_limit_bytes=12 * 1024 * 1024),
        cost_estimate=pl.CostEstimate(
            flops=32 * rows * columns * rank, bytes_accessed=4 * rows * columns, transcendentals=0
        ),
    )(*map(in_hbm, (train_gate, train_up, low_gate_t, low_up_t, gain, high_gate, high_up)))


def write_rows(stage, slot, out_hbm, start, size, sem):
    return pltpu.make_async_copy(stage.at[pl.ds(slot, size), :], out_hbm.at[pl.ds(start, size), :], sem)


def scale_partner(
    raw, adapter, gain_rows, gain_at, scale, stage, slot, out_hbm, start, sems, sem_at, group=UNROLL, block=BLOCK
):
    size, columns = raw.shape
    block = min(block, size)
    tile = min(TILE, columns)

    def merge(i):
        at = pl.multiple_of(i * block, block)
        gain_block = gain_rows[pl.ds(gain_at + at, block), :]
        for c in range(0, columns, tile):
            value = gained_tile(raw[pl.ds(at, block), c : c + tile], adapter(at, block, c, tile), gain_block)
            scaled = value.reshape(block // 8, 8, tile) * scale[:, c : c + tile][None]
            stage[pl.ds(slot + at, block), c : c + tile] = scaled.reshape(block, tile).astype(jnp.bfloat16)

    def send(i):
        at = pl.multiple_of(i * block, block)
        write_rows(stage, slot + at, out_hbm, start + at, block, sems.at[sem_at + i]).start()

    def merge_and_send(i):
        merge(i)
        send(i)

    in_groups(size // block, group, merge_and_send)


def scale_own(gained, scale, stage, slot, out_hbm, start, sems, sem_at):
    size, columns = gained.shape
    block = min(BLOCK, size)
    tile = min(TILE, columns)

    @pl.loop(0, size // block)
    def _(i):
        at = pl.multiple_of(i * block, block)
        for c in range(0, columns, tile):
            value = gained[pl.ds(at, block), c : c + tile].reshape(block // 8, 8, tile)
            scaled = (value * scale[:, c : c + tile][None]).reshape(block, tile)
            stage[pl.ds(slot + at, block), c : c + tile] = scaled.astype(jnp.bfloat16)
        write_rows(stage, slot + at, out_hbm, start + at, block, sems.at[sem_at + i]).start()


def wait_rows(stage, slot, out_hbm, start, size, sems, sem_at, block=BLOCK):
    block = min(block, size)

    @pl.loop(0, size // block)
    def _(i):
        at = pl.multiple_of(i * block, block)
        write_rows(stage, slot + at, out_hbm, start + at, block, sems.at[sem_at + i]).wait()


def first_kernel(parts, *refs):
    gained_gate, gained_up, high_gate, high_up = refs[:4]
    news = refs[4 : 4 + parts]
    others = parts - 1
    raws = refs[4 + parts : 4 + parts + others]
    lows = refs[4 + parts + others : 4 + parts + 2 * others]
    rest = refs[4 + parts + 2 * others :]
    ready_gate, ready_up, column_gate, column_up, product_up, gain_rows, scale_up = rest[:7]
    scale_gate, low_gate_rows, low_up_rows, stage, sems = rest[7:]
    rows, columns = gained_gate.shape
    block = min(BLOCK, rows)
    blocks = rows // block
    tile = min(TILE, columns)
    me = lax.axis_index("fsdp")

    for at, column, scale in ((0, column_gate, scale_gate), (columns, column_up, scale_up)):
        best = news[0][:, at : at + columns]
        for new in news[1:]:
            best = jnp.maximum(best, new[:, at : at + columns])
        column[...] = best
        scale[...] = jnp.broadcast_to(1.0 / best, (8, columns))

    start = pl.multiple_of(me * rows, rows)
    scale_own(gained_gate, scale_gate, stage, 0, ready_gate, start, sems, 0)
    scale_own(gained_up, scale_up, stage, parts * rows, ready_up, start, sems, parts * blocks)
    for k in range(others):
        spread_rows(lows[k][:, :rows], news[k + 1][:, 2 * columns :], low_gate_rows, gain_rows, k * rows)
        spread_rows(lows[k][:, rows:], None, low_up_rows, gain_rows, k * rows)
        there = pl.multiple_of(lax.rem(me - (k + 1) + parts, parts) * rows, rows)
        scale_partner(
            raws[k], multiplied(low_gate_rows.at[pl.ds(k * rows, rows), :], high_gate), gain_rows, k * rows, scale_gate,
            stage, (k + 1) * rows, ready_gate, there, sems, (k + 1) * blocks,
        )

    def product(n):
        c = pl.multiple_of(n * tile, tile)
        product_up[:, pl.ds(c, tile)] = jnp.dot(
            low_up_rows[...], high_up[:, pl.ds(c, tile)], preferred_element_type=jnp.float32
        )

    in_groups(columns // tile, PRODUCTS, product)
    wait_rows(stage, 0, ready_gate, start, rows, sems, 0)
    for k in range(others):
        there = pl.multiple_of(lax.rem(me - (k + 1) + parts, parts) * rows, rows)
        wait_rows(stage, (k + 1) * rows, ready_gate, there, rows, sems, (k + 1) * blocks)
    wait_rows(stage, parts * rows, ready_up, start, rows, sems, parts * blocks)


def first(gained_gate, gained_up, news, raws, lows, high_gate, high_up):
    parts = len(news)
    others = parts - 1
    rows, columns = gained_gate.shape
    rank = high_gate.shape[0]
    blocks = rows // min(BLOCK, rows)
    return pl.pallas_call(
        functools.partial(first_kernel, parts),
        out_shape=(
            pltpu.HBM((parts * rows, columns), jnp.bfloat16),
            pltpu.HBM((parts * rows, columns), jnp.bfloat16),
            jax.ShapeDtypeStruct((1, columns), jnp.float32),
            jax.ShapeDtypeStruct((1, columns), jnp.float32),
            pltpu.VMEM((others * rows, columns), jnp.float32),
            pltpu.VMEM((others * rows, 128), jnp.float32),
            pltpu.VMEM((8, columns), jnp.float32),
        ),
        in_specs=[VMEM_SPEC] * (4 + parts + 2 * others),
        out_specs=(HBM_SPEC, HBM_SPEC) + (VMEM_SPEC,) * 5,
        scratch_shapes=[
            pltpu.VMEM((8, columns), jnp.float32),
            pltpu.VMEM((others * rows, rank), jnp.bfloat16),
            pltpu.VMEM((others * rows, rank), jnp.bfloat16),
            pltpu.VMEM(((parts + 1) * rows, columns), jnp.bfloat16),
            pltpu.SemaphoreType.DMA(((parts + 1) * blocks,)),
        ],
        compiler_params=pltpu.CompilerParams(vmem_limit_bytes=18 * 1024 * 1024),
        cost_estimate=pl.CostEstimate(
            flops=16 * parts * rows * columns * rank, bytes_accessed=4 * parts * rows * columns, transcendentals=0
        ),
    )(
        in_vmem(gained_gate), in_vmem(gained_up), in_vmem(high_gate), in_vmem(high_up),
        *map(in_vmem, news), *map(in_vmem, raws), *map(in_vmem, lows),
    )


def later_kernel(parts, rows, offset, *refs):
    others = parts - 1
    raws = refs[:others]
    product, gain_rows, scale, _, ready, stage, sems = refs[others:]
    size = raws[0].shape[0]
    blocks = size // min(LATER_BLOCK, size)
    me = lax.axis_index("fsdp")
    for k in range(others):
        there = pl.multiple_of(lax.rem(me - (k + 1) + parts, parts) * rows + offset, min(LATER_BLOCK, size))

        def added(at, block, c, tile, k=k):
            return product[pl.ds(k * rows + offset + at, block), c : c + tile]

        scale_partner(
            raws[k], added, gain_rows, k * rows + offset, scale,
            stage, k * size, ready, there, sems, k * blocks, LATER_UNROLL, LATER_BLOCK,
        )
    for k in range(others):
        there = pl.multiple_of(lax.rem(me - (k + 1) + parts, parts) * rows + offset, min(LATER_BLOCK, size))
        wait_rows(stage, k * size, ready, there, size, sems, k * blocks, LATER_BLOCK)


def later(ready, raws, product, gain_rows, scale, rows, offset):
    others = len(raws)
    size, columns = raws[0].shape
    blocks = size // min(LATER_BLOCK, size)
    return pl.pallas_call(
        functools.partial(later_kernel, others + 1, rows, offset),
        out_shape=pltpu.HBM(ready.shape, ready.dtype),
        in_specs=[VMEM_SPEC] * (others + 3) + [HBM_SPEC],
        out_specs=HBM_SPEC,
        input_output_aliases={others + 3: 0},
        scratch_shapes=[
            pltpu.VMEM((others * size, columns), jnp.bfloat16),
            pltpu.SemaphoreType.DMA((others * blocks,)),
        ],
        compiler_params=pltpu.CompilerParams(vmem_limit_bytes=8 * 1024 * 1024),
        cost_estimate=pl.CostEstimate(
            flops=256 * others * size * columns, bytes_accessed=4 * others * size * columns, transcendentals=0
        ),
    )(*map(in_vmem, raws), in_vmem(product), in_vmem(gain_rows), in_vmem(scale), in_hbm(ready))


def chunks_of(rows):
    return ((0, rows),)


def solution(mesh):
    parts = mesh.shape["fsdp"]

    def around(x):
        return [
            lax.ppermute(x, "fsdp", [(i, (i + k) % parts) for i in range(parts)]) for k in range(1, parts)
        ]

    def per_device(train_gate, low_gate, high_gate, train_up, low_up, high_up, norm_gain):
        rows = train_gate.shape[0]
        chunks = chunks_of(rows)
        gates = around(train_gate)
        gained_gate, gained_up, new, low, high_gate, high_up, *pieces = own(
            train_gate, train_up, low_gate.T, low_up.T, norm_gain.reshape(1, -1), high_gate, high_up, chunks
        )
        news = [new] + around(new)
        lows = around(low)
        ups = [around(piece) for piece in pieces]
        ready_gate, ready_up, column_gate, column_up, product_up, gain_rows, scale_up = first(
            gained_gate, gained_up, news, gates, lows, high_gate, high_up
        )
        for n, (offset, _) in enumerate(chunks):
            ready_up = later(ready_up, ups[n], product_up, gain_rows, scale_up, rows, offset)
        return ready_gate, ready_up, column_gate.reshape(-1), column_up.reshape(-1)

    placed = (
        P(("trial", "fsdp"), "cols"),
        P(("trial", "fsdp"), None),
        P("trial", "cols"),
        P(("trial", "fsdp"), "cols"),
        P(("trial", "fsdp"), None),
        P("trial", "cols"),
        P(("trial", "fsdp")),
    )
    return jax.shard_map(
        per_device,
        mesh=mesh,
        in_specs=placed,
        out_specs=(
            P("trial", "cols"),
            P("trial", "cols"),
            P(("trial", "cols")),
            P(("trial", "cols")),
        ),
        check_vma=False,
    )
```
